32 devices in a mesh: node: 4 (over z), local: 8 (over y, x, core).
Axes of the slice: x: 2, y: 2, z: 4, core: 2. Of those that a mesh axis runs over, the one named last changes fastest.
Arguments:
- tokens: bfloat16 [512, 7168], P(('node', 'local')), may hold values from -6 to 6
- grad_out: bfloat16 [512, 7168], P(('node', 'local')), may hold values from -6 to 6
- gates: bfloat16 [512, 3], P(('node', 'local')), may hold values from 0.19921875 to 1
- expert_ids: int32 [512, 3], P(('node', 'local')), may hold values from 0 to 7, as said below
- w_gate: bfloat16 [4, 7168, 2048], P('node', None, 'local'), may hold values from -0.0625 to 0.0625
- w_up: bfloat16 [4, 7168, 2048], P('node', None, 'local'), may hold values from -0.0625 to 0.0625
- w_down: bfloat16 [4, 7168, 2048], P('node', None, 'local'), may hold values from -0.1875 to 0.1875
- s_gate: bfloat16 [7168, 2048], P(None, 'local'), may hold values from -0.0625 to 0.0625
- s_up: bfloat16 [7168, 2048], P(None, 'local'), may hold values from -0.0625 to 0.0625
- s_down: bfloat16 [7168, 2048], P(None, 'local'), may hold values from -0.125 to 0.125
Outputs:
- dx: bfloat16 [512, 7168], P(('node', 'local'))
- dgates: float32 [512, 3], P(('node', 'local'))
- d_w_gate: bfloat16 [4, 7168, 2048], P('node', None, 'local')
- d_w_up: bfloat16 [4, 7168, 2048], P('node', None, 'local')
- d_w_down: bfloat16 [4, 7168, 2048], P('node', None, 'local')
- d_s_gate: bfloat16 [7168, 2048], P('node', 'local')
- d_s_up: bfloat16 [7168, 2048], P('node', 'local')
- d_s_down: bfloat16 [7168, 2048], P('node', 'local')
The draws below stay inside these ranges and needn't reach their ends.
Inputs may be any that keep to these rules, and one draw needn't show every extreme that they name: `expert_ids`: each token names both experts of one node and one expert of a second node. Of the tokens of one device exactly 8 name experts of each node and at most 8 name any one expert; for every node one of its experts is named by exactly 8 tokens of every device.
All inputs are finite; a program needn't handle non-finite values.
Results may differ from the reference program's by a relative error of at most 0.014.
Values may be sent and summed in bfloat16 or wider, within the bound.
A program may use at most 192 MiB of HBM per device.

```python
import jax
import jax.numpy as jnp
from jax import lax

D = 7168
FF = 1024
FFS = 2048
TOPK = 3
E_NODE = 2
TOK_DEV = 16
TOKENS = 512
EXPERTS = 8
N_NODE = 4
N_LOCAL = 8


def draw_expert_ids(key, part):
    node_count = EXPERTS // E_NODE
    device_count = TOKENS // TOK_DEV
    keys = jax.random.split(key, 4)
    node_order = jax.vmap(lambda item: jax.random.permutation(item, node_count))(jax.random.split(keys[0], device_count))
    position = jnp.arange(TOK_DEV, dtype=jnp.int32)
    first_slot = position % node_count
    second_slot = (first_slot + 1 + position // node_count % (node_count - 1)) % node_count
    first = jnp.take(node_order, first_slot, axis=1)
    second = jnp.take(node_order, second_slot, axis=1)
    busy = jax.random.randint(keys[1], (node_count,), 0, E_NODE)
    single = jnp.take(busy, second)
    trio = jnp.stack([first * E_NODE, first * E_NODE + 1, second * E_NODE + single], axis=-1)
    shift = jax.random.randint(keys[2], (device_count, TOK_DEV, 1), 0, 3)
    column = (jnp.arange(3, dtype=jnp.int32)[None, None, :] + shift) % 3
    trio = jnp.take_along_axis(trio, column, axis=2)
    shuffle = jax.vmap(lambda item: jax.random.permutation(item, TOK_DEV))(jax.random.split(keys[3], device_count))
    trio = jnp.take_along_axis(trio, shuffle[:, :, None], axis=1)
    return trio.reshape(TOKENS, 3).astype(jnp.int32)


def shard_levels(stream_key, extent, shards, least, top_value):
    loudness, own = 1.0, jax.random.fold_in(stream_key, 6)
    for dim, blocks in shards:
        heights = jnp.exp(jax.random.uniform(jax.random.fold_in(own, dim), (blocks,), jnp.float32, least / len(shards), top_value / len(shards)))
        loudness = loudness * jnp.repeat(heights, extent[dim] // blocks).reshape([-1 if axis == dim else 1 for axis in range(len(extent))])
    return loudness


def bell_draw(own_key, extent, deviation, bound, shards=(), kind=jnp.bfloat16):
    factor_of = shard_levels(own_key, extent, shards, -0.22, 0.18) if shards else 1.0
    array = jax.random.normal(own_key, extent, jnp.float32) * deviation * factor_of
    return jnp.minimum(jnp.maximum(array, -bound), bound).astype(kind)


def setup_inputs(seed: int = 0) -> dict:
    key_of = jax.random.split(jax.random.key(seed), 11)
    tokens = bell_draw(key_of[0], (TOKENS, D), 1.0, 6.0, ((0, 32),))
    grad_out = bell_draw(key_of[1], (TOKENS, D), 1.0, 6.0, ((0, 32),))
    gates = jnp.clip(0.19921875 + 0.80078125 * jax.random.uniform(key_of[2], (TOKENS, TOPK), jnp.float32) ** shard_levels(key_of[2], (TOKENS, TOPK), ((0, 32),), -0.2, 0.2), 0.19921875, 1.0).astype(jnp.bfloat16)
    expert_ids = draw_expert_ids(jax.random.fold_in(key_of[10], 71), 0)
    w_gate = bell_draw(key_of[4], (N_NODE, D, E_NODE * FF), D ** -0.5, 0.0625, ((0, 4), (2, 8)))
    w_up = bell_draw(key_of[5], (N_NODE, D, E_NODE * FF), D ** -0.5, 0.0625, ((0, 4), (2, 8)))
    w_down = bell_draw(key_of[6], (N_NODE, D, E_NODE * FF), FF ** -0.5, 0.1875, ((0, 4), (2, 8)))
    s_gate = bell_draw(key_of[7], (D, FFS), D ** -0.5, 0.0625, ((1, 8),))
    s_up = bell_draw(key_of[8], (D, FFS), D ** -0.5, 0.0625, ((1, 8),))
    s_down = bell_draw(key_of[9], (D, FFS), FFS ** -0.5, 0.125, ((1, 8),))
    return {"tokens": tokens, "grad_out": grad_out, "gates": gates, "expert_ids": expert_ids, "w_gate": w_gate, "w_up": w_up, "w_down": w_down, "s_gate": s_gate, "s_up": s_up, "s_down": s_down}


def silu_parts(pre_gate):
    sig = jax.nn.sigmoid(pre_gate)
    return pre_gate * sig, sig * (1.0 + pre_gate * (1.0 - sig))


def contract_first(left, right):
    return lax.dot_general(left, right, (((0,), (0,)), ((), ())), preferred_element_type=jnp.float32)


def contract_last(left, right):
    return lax.dot_general(left, right, (((1,), (1,)), ((), ())), preferred_element_type=jnp.float32)


def ffn_backward(rows_in, rows_grad, weight, gate_w, up_w, down_w):
    pre_gate = jnp.dot(rows_in, gate_w, preferred_element_type=jnp.float32)
    pre_up = jnp.dot(rows_in, up_w, preferred_element_type=jnp.float32)
    activ, slope = silu_parts(pre_gate)
    hidden = activ * pre_up
    upstream = jnp.dot(rows_grad, down_w, preferred_element_type=jnp.float32)
    scaled = weight * upstream
    grad_up = (scaled * activ).astype(jnp.bfloat16)
    grad_gate = (scaled * pre_up * slope).astype(jnp.bfloat16)
    weighted = (weight * hidden).astype(jnp.bfloat16)
    return grad_gate, grad_up, weighted, hidden * upstream


def block_rows(grad_gate, grad_up, gate_w, up_w, width):
    blocks = gate_w.shape[1] // width

    def step(index, total):
        start = index * width
        part = contract_last(lax.dynamic_slice_in_dim(grad_gate, start, width, 1), lax.dynamic_slice_in_dim(gate_w, start, width, 1))
        part = part + contract_last(lax.dynamic_slice_in_dim(grad_up, start, width, 1), lax.dynamic_slice_in_dim(up_w, start, width, 1))
        rounded = lax.optimization_barrier(part.astype(jnp.bfloat16))
        return total + rounded.astype(jnp.float32)

    return lax.fori_loop(0, blocks, step, jnp.zeros((grad_gate.shape[0], gate_w.shape[0]), jnp.float32))


def block_stat(product, width):
    sums = jnp.sum(product.reshape(product.shape[0], -1, width), axis=2)
    return jnp.sum(lax.optimization_barrier(sums.astype(jnp.bfloat16)).astype(jnp.float32), axis=1)


def reference(tokens, grad_out, gates, expert_ids, w_gate, w_up, w_down, s_gate, s_up, s_down):
    n_tok = tokens.shape[0]
    width = tokens.shape[1]
    device_count = n_tok // TOK_DEV
    slots = device_count * (2 * TOK_DEV // N_NODE)
    group_size = N_LOCAL // E_NODE
    ff_block = FF // group_size
    gate_all = gates.astype(jnp.float32)
    positions = jnp.arange(n_tok, dtype=jnp.int32)

    def per_expert(carry, expert):
        dx_acc, dgate_acc = carry
        chosen = expert_ids == expert
        member = jnp.any(chosen, axis=1)
        weight = jnp.sum(jnp.where(chosen, gate_all, 0.0), axis=1)
        ranking = jnp.cumsum(member.astype(jnp.int32)) - 1
        target = jnp.where(member, ranking, slots).astype(jnp.int32)
        index = jnp.zeros((slots + 1,), jnp.int32).at[target].set(positions)[:slots]
        valid = jnp.zeros((slots + 1,), jnp.float32).at[target].set(1.0)[:slots]
        rows_in = tokens[index]
        rows_grad = grad_out[index]
        row_weight = (weight[index] * valid)[:, None]
        node = expert // E_NODE
        column = (expert % E_NODE) * FF
        gate_w = lax.dynamic_slice_in_dim(lax.dynamic_index_in_dim(w_gate, node, 0, keepdims=False), column, FF, 1)
        up_w = lax.dynamic_slice_in_dim(lax.dynamic_index_in_dim(w_up, node, 0, keepdims=False), column, FF, 1)
        down_w = lax.dynamic_slice_in_dim(lax.dynamic_index_in_dim(w_down, node, 0, keepdims=False), column, FF, 1)
        grad_gate, grad_up, weighted, product = ffn_backward(rows_in, rows_grad, row_weight, gate_w, up_w, down_w)
        partial_value = block_rows(grad_gate, grad_up, gate_w, up_w, ff_block)
        stat = block_stat(product, ff_block)
        dx_acc = dx_acc.at[index].add(partial_value * valid[:, None])
        token_stat = jnp.zeros((n_tok,), jnp.float32).at[index].add(stat * valid)
        dgate_acc = dgate_acc + jnp.where(chosen, token_stat[:, None], 0.0)
        grads = (contract_first(rows_in, grad_gate).astype(jnp.bfloat16), contract_first(rows_in, grad_up).astype(jnp.bfloat16), contract_first(rows_grad, weighted).astype(jnp.bfloat16))
        return (dx_acc, dgate_acc), grads

    start_carry = (jnp.zeros((n_tok, width), jnp.float32), jnp.zeros(expert_ids.shape, jnp.float32))
    (dx_routed, dgates), stacked = lax.scan(per_expert, start_carry, jnp.arange(E_NODE * N_NODE, dtype=jnp.int32))

    def arrange(grad):
        shaped = grad.reshape(N_NODE, E_NODE, width, FF)
        return jnp.transpose(shaped, (0, 2, 1, 3)).reshape(N_NODE, width, E_NODE * FF)

    unit_weight = jnp.ones((n_tok, 1), jnp.float32)
    grad_gate, grad_up, weighted, product = ffn_backward(tokens, grad_out, unit_weight, s_gate, s_up, s_down)
    dx_shared = block_rows(grad_gate, grad_up, s_gate, s_up, FFS // N_LOCAL)
    per_node = n_tok // N_NODE

    def node_step(index, totals):
        start = index * per_node
        rows_in = lax.dynamic_slice_in_dim(tokens, start, per_node, 0)
        rows_grad = lax.dynamic_slice_in_dim(grad_out, start, per_node, 0)
        parts = (contract_first(rows_in, lax.dynamic_slice_in_dim(grad_gate, start, per_node, 0)), contract_first(rows_in, lax.dynamic_slice_in_dim(grad_up, start, per_node, 0)), contract_first(rows_grad, lax.dynamic_slice_in_dim(weighted, start, per_node, 0)))
        return tuple(total + lax.optimization_barrier(part.astype(jnp.bfloat16)).astype(jnp.float32) for total, part in zip(totals, parts))

    empty = jnp.zeros((width, FFS), jnp.float32)
    shared = lax.fori_loop(0, N_NODE, node_step, (empty, empty, empty))
    dx = (dx_routed + dx_shared).astype(jnp.bfloat16)
    return (dx, dgates, arrange(stacked[0]), arrange(stacked[1]), arrange(stacked[2]), shared[0].astype(jnp.bfloat16), shared[1].astype(jnp.bfloat16), shared[2].astype(jnp.bfloat16))
```

```python
import functools

import jax
import jax.numpy as jnp
from jax import lax
from jax.experimental import pallas as pl
from jax.experimental.pallas import tpu as pltpu
from jax.sharding import PartitionSpec as P

E_NODE = 2
LANES = 128
MESH = pl.DeviceIdType.MESH


def bit_orders(local_count):
    bits = local_count.bit_length() - 1
    outer = list(range(1, bits))
    forward = [1 << b for b in outer] + [1]
    backward = [1 << b for b in outer[::-1]] + [1]
    return (forward, backward)


def near_first(node_count):
    return sorted(range(1, node_count), key=lambda s: min(s, node_count - s))


def greet(node_count, masks):
    n, l = lax.axis_index("node"), lax.axis_index("local")
    barrier = pltpu.get_barrier_semaphore()
    for r in range(1, node_count):
        pl.semaphore_signal(
            barrier, inc=1, device_id=(lax.rem(n + r, node_count), l), device_id_type=MESH
        )
    for mask in masks:
        pl.semaphore_signal(barrier, inc=1, device_id=(n, l ^ mask), device_id_type=MESH)
    pl.semaphore_wait(barrier, node_count - 1 + len(masks))


def gather_kernel(
    node_count, orders, tok, grad, sel_t, sel_g, meta,
    all_t, all_g, ext_t, ext_g, all_m, send_sem, recv_sem, own_sem,
):
    n, l = lax.axis_index("node"), lax.axis_index("local")
    forward, backward = orders
    stages = len(forward)
    own_blocks = tok.shape[0]
    part = ext_t.shape[-1]
    greet(node_count, forward)
    counter = [0]
    sends = []

    def remote(src, dst, device):
        i = counter[0]
        counter[0] += 1
        copy = pltpu.make_async_remote_copy(
            src_ref=src, dst_ref=dst, send_sem=send_sem.at[i], recv_sem=recv_sem.at[i],
            device_id=device, device_id_type=MESH,
        )
        copy.start()
        sends.append(copy)
        return copy

    fills = [
        pltpu.make_async_copy(tok, all_t.at[0, pl.ds(0, own_blocks)], own_sem.at[0]),
        pltpu.make_async_copy(grad, all_g.at[0, pl.ds(0, own_blocks)], own_sem.at[1]),
        pltpu.make_async_copy(meta.at[0], all_m.at[0, 0], own_sem.at[2]),
    ]
    for fill in fills:
        fill.start()

    def view(buf, s, start, size):
        if buf is all_t or buf is all_g:
            if s == 0:
                return buf.at[pl.ds(start, size), pl.ds(0, own_blocks)]
            return buf.at[pl.ds(start, size), own_blocks + s - 1]
        if buf is all_m:
            return buf.at[s, pl.ds(start, size)]
        return buf.at[s - 1, pl.ds(start, size)]

    arrived = {}
    order = near_first(node_count)
    for s in order:
        r = node_count - s
        m = lax.rem(n + r, node_count)
        columns = pl.ds(pl.multiple_of(m * part, LANES), part)
        arrived[s] = [
            remote(meta.at[r], all_m.at[s, 0], (m, l)),
            remote(sel_t.at[r - 1], all_t.at[0, own_blocks + s - 1], (m, l)),
            remote(sel_g.at[r - 1], all_g.at[0, own_blocks + s - 1], (m, l)),
            remote(tok.at[:, :, columns], ext_t.at[s - 1, 0], (m, l)),
            remote(grad.at[:, :, columns], ext_g.at[s - 1, 0], (m, l)),
        ]
    for fill in fills:
        fill.wait()

    items = [0] + order
    pending = {}

    def issue(item, stage):
        s = items[item]
        bufs = [(all_m, forward), (all_t, forward), (all_g, backward)]
        if s > 0:
            bufs += [(ext_t, forward), (ext_g, backward)]
        if stage > 0:
            before = pending[item]
        else:
            before = arrived.get(s, [])
        for copy in before:
            copy.wait_recv()
        size = 1 << stage
        pending[item] = [
            remote(view(buf, s, 0, size), view(buf, s, size, size), (n, l ^ bits[stage]))
            for buf, bits in bufs
        ]

    for tick in range(len(items) + stages - 1):
        for item in range(len(items)):
            stage = tick - item
            if 0 <= stage < stages:
                issue(item, stage)
    for item in range(len(items)):
        for copy in pending[item]:
            copy.wait_recv()
    for copy in sends:
        copy.wait_send()


def gather_rows(node_count, local_count, tok, grad, sel_t, sel_g, meta):
    own_blocks, cap, width = tok.shape
    orders = bit_orders(local_count)
    part = width // node_count
    copies = len(orders[0]) * (3 + 5 * (node_count - 1)) + 5 * (node_count - 1)
    rows = (local_count, own_blocks + node_count - 1, cap, width)
    ext = (node_count - 1, local_count, own_blocks, cap, part)
    bf16 = jnp.bfloat16
    vmem = pl.BlockSpec(memory_space=pltpu.VMEM)
    hbm = pl.BlockSpec(memory_space=pl.ANY)
    return pl.pallas_call(
        functools.partial(gather_kernel, node_count, orders),
        out_shape=[
            jax.ShapeDtypeStruct(rows, bf16),
            jax.ShapeDtypeStruct(rows, bf16),
            jax.ShapeDtypeStruct(ext, bf16),
            jax.ShapeDtypeStruct(ext, bf16),
            jax.ShapeDtypeStruct((node_count, local_count) + meta.shape[1:], bf16),
        ],
        in_specs=[vmem] * 5,
        out_specs=[hbm] * 5,
        scratch_shapes=[
            pltpu.SemaphoreType.DMA((copies,)),
            pltpu.SemaphoreType.DMA((copies,)),
            pltpu.SemaphoreType.DMA((3,)),
        ],
        compiler_params=pltpu.CompilerParams(collective_id=0, has_side_effects=True),
        name="gather_rows",
    )(tok, grad, sel_t, sel_g, meta)


def reduce_kernel(node_count, forward, own_blocks, part_ref, own_ref, home_ref,
                  acc, land, back, send_sem, recv_sem, zsend_sem, zrecv_sem, load_sem):
    n, l = lax.axis_index("node"), lax.axis_index("local")
    count, blocks, cap, width = part_ref.shape
    stages = len(forward)
    half = width // 2 // LANES * LANES
    load = pltpu.make_async_copy(part_ref, acc, load_sem)
    load.start()
    greet(node_count, forward)
    load.wait()
    groups = [(own_blocks, blocks - own_blocks), (0, own_blocks)]
    bands = [(0, half), (half, width - half)]
    top = stages - 1
    plans = [[top] + list(range(top))[::-1], [top] + list(range(top))]
    counter = [0]
    sends = []
    keep = {key: list(range(count)) for key in [(g, b) for g in range(2) for b in range(2)]}
    flight = {}

    def start(g, b, stage):
        bit = 1 << plans[b][stage]
        first, size = groups[g]
        columns = pl.ds(*bands[b])
        out = [p for p in keep[g, b] if p & bit]
        stay = [p for p in keep[g, b] if not p & bit]
        keep[g, b] = stay
        copies = []
        for p in out:
            i = counter[0]
            counter[0] += 1
            copy = pltpu.make_async_remote_copy(
                src_ref=acc.at[p, pl.ds(first, size), :, columns],
                dst_ref=land.at[p, pl.ds(first, size), :, columns],
                send_sem=send_sem.at[i], recv_sem=recv_sem.at[i],
                device_id=(n, l ^ forward[plans[b][stage]]), device_id_type=MESH,
            )
            copy.start()
            sends.append(copy)
            copies.append((p, copy))
        flight[g, b] = (bit, copies)

    def settle(g, b):
        first, size = groups[g]
        columns = pl.ds(*bands[b])
        bit, copies = flight[g, b]
        for p, copy in copies:
            copy.wait_recv()
            q = p ^ bit

            def add(k, carry, p=p, q=q):
                there = land[p, first + k, :, columns].astype(jnp.float32)
                here = acc[q, first + k, :, columns].astype(jnp.float32)
                acc[q, first + k, :, columns] = (here + there).astype(jnp.bfloat16)
                return carry

            lax.fori_loop(0, size, add, 0)

    homes = []
    for stage in range(stages + 1):
        for g in range(2):
            for b in range(2):
                if stage > 0:
                    settle(g, b)
                if stage < stages:
                    start(g, b, stage)
            if stage == stages and g == 0:
                for s in near_first(node_count):
                    copy = pltpu.make_async_remote_copy(
                        src_ref=acc.at[0, own_blocks + s - 1],
                        dst_ref=back.at[node_count - s - 1],
                        send_sem=zsend_sem.at[s - 1],
                        recv_sem=zrecv_sem.at[node_count - s - 1],
                        device_id=(lax.rem(n + s, node_count), l), device_id_type=MESH,
                    )
                    copy.start()
                    homes.append(copy)
    own_ref[...] = acc[0, pl.ds(0, own_blocks)]
    for copy in homes:
        copy.wait_recv()
    home_ref[...] = back[...]
    for copy in sends + homes:
        copy.wait_send()


def reduce_rows(node_count, local_count, part):
    count, blocks, cap, width = part.shape
    forward = bit_orders(local_count)[0]
    own_blocks = blocks - (node_count - 1)
    bf16 = jnp.bfloat16
    vmem = pl.BlockSpec(memory_space=pltpu.VMEM)
    copies = 4 * (local_count - 1)
    return pl.pallas_call(
        functools.partial(reduce_kernel, node_count, forward, own_blocks),
        out_shape=[
            jax.ShapeDtypeStruct((own_blocks, cap, width), bf16),
            jax.ShapeDtypeStruct((node_count - 1, cap, width), bf16),
        ],
        in_specs=[pl.BlockSpec(memory_space=pl.ANY)],
        out_specs=[vmem] * 2,
        scratch_shapes=[
            pltpu.VMEM(part.shape, bf16),
            pltpu.VMEM(part.shape, bf16),
            pltpu.VMEM((node_count - 1, cap, width), bf16),
            pltpu.SemaphoreType.DMA((copies,)),
            pltpu.SemaphoreType.DMA((copies,)),
            pltpu.SemaphoreType.DMA((node_count - 1,)),
            pltpu.SemaphoreType.DMA((node_count - 1,)),
            pltpu.SemaphoreType.DMA,
        ],
        compiler_params=pltpu.CompilerParams(collective_id=1, has_side_effects=True),
        name="reduce_rows",
    )(part)


def silu_parts(pre_gate):
    sig = jax.nn.sigmoid(pre_gate)
    return (pre_gate * sig, sig * (1.0 + pre_gate * (1.0 - sig)))


def dot(left, right):
    return jnp.dot(left, right, preferred_element_type=jnp.float32)


def contract_first(left, right):
    return lax.dot_general(
        left, right, (((0,), (0,)), ((), ())), preferred_element_type=jnp.float32
    )


def contract_last(left, right):
    return lax.dot_general(
        left, right, (((1,), (1,)), ((), ())), preferred_element_type=jnp.float32
    )


def flip(values, local_count):
    bits = local_count.bit_length() - 1
    shaped = values.reshape((2,) * bits + (-1,) + values.shape[1:])
    axes = (0,) + tuple(range(1, bits))[::-1] + tuple(range(bits, shaped.ndim))
    return jnp.transpose(shaped, axes).reshape(values.shape)


def ffn_backward(pre_gate, pre_up, upstream, weight):
    activ, slope = silu_parts(pre_gate)
    hidden = activ * pre_up
    scaled = weight * upstream
    grad_up = (scaled * activ).astype(jnp.bfloat16)
    grad_gate = (scaled * pre_up * slope).astype(jnp.bfloat16)
    weighted = (weight * hidden).astype(jnp.bfloat16)
    return (grad_gate, grad_up, weighted, hidden * upstream)


def local(tokens, grad_out, gates, expert_ids, w_gate, w_up, w_down, s_gate, s_up, s_down):
    held, width = tokens.shape
    nodes, locals_ = lax.axis_size("node"), lax.axis_size("local")
    n, l = lax.axis_index("node"), lax.axis_index("local")
    cap = 2 * held // nodes
    own_blocks = held // cap
    bf16, f32 = jnp.bfloat16, jnp.float32

    rel = lax.rem(expert_ids // E_NODE - n + nodes, nodes)
    near = jnp.arange(nodes, dtype=jnp.int32)
    hit_k = rel[:, :, None] == near
    hit = jnp.any(hit_k, axis=1)
    lower = jnp.tril(jnp.ones((held, held), f32))
    rank = dot(lower, hit.astype(f32)).astype(jnp.int32) - 1
    slots = jnp.arange(cap, dtype=jnp.int32)
    pick = hit[:, :, None] & (rank[:, :, None] == slots)
    which = (lax.rem(expert_ids, E_NODE)[:, :, None] == jnp.arange(E_NODE)) & True
    named = hit_k[:, :, :, None] & which[:, :, None, :]
    weight = jnp.sum(jnp.where(named, gates.astype(f32)[:, :, None, None], 0.0), axis=1)
    rows = pick[:, 1:].astype(bf16)
    sel_t = jnp.einsum("trc,td->rcd", rows, tokens, preferred_element_type=f32).astype(bf16)
    sel_g = jnp.einsum("trc,td->rcd", rows, grad_out, preferred_element_type=f32).astype(bf16)
    slot_w = jnp.sum(jnp.where(pick[:, 1:, :, None], weight[:, 1:, None, :], 0.0), axis=0)
    meta = jnp.zeros((nodes, held, LANES), f32)
    meta = meta.at[0, :, :E_NODE].set(weight[:, 0])
    meta = meta.at[1:, :cap, :E_NODE].set(slot_w).astype(bf16)

    all_t, all_g, ext_t, ext_g, all_m = gather_rows(
        nodes, locals_,
        tokens.reshape(own_blocks, cap, width), grad_out.reshape(own_blocks, cap, width),
        sel_t, sel_g, meta,
    )
    total = locals_ * (held + (nodes - 1) * cap)
    rows_t, rows_g = all_t.reshape(total, width), all_g.reshape(total, width)
    units = s_gate.shape[1]

    def own(values):
        return values.reshape(locals_, -1, values.shape[-1])[:, :held].reshape(
            locals_ * held, values.shape[-1]
        )

    pre_gate, pre_up = dot(rows_t, s_gate), dot(rows_t, s_up)
    upstream = flip(dot(rows_g, s_down), locals_)
    sg, su, sh, _ = ffn_backward(own(pre_gate), own(pre_up), own(upstream), 1.0)
    pack = jnp.concatenate([sg, su, flip(sh, locals_)], axis=1)
    packs = [pack] + [
        lax.ppermute(pack, "node", [((i + s) % nodes, i) for i in range(nodes)])
        for s in range(1, nodes)
    ]

    expert = l // (locals_ // E_NODE)
    table = jnp.concatenate([all_m[0, :, :, :E_NODE]] + [
        all_m[s, :, :cap, :E_NODE] for s in range(1, nodes)
    ], axis=1).reshape(total, E_NODE).astype(f32)
    mine = jnp.arange(E_NODE) == expert
    row_w = jnp.sum(jnp.where(mine, table, 0.0), axis=1, keepdims=True)
    gate_w, up_w, down_w = w_gate[0], w_up[0], w_down[0]
    gg, gu, gh, product = ffn_backward(
        dot(rows_t, gate_w), dot(rows_t, up_w), flip(dot(rows_g, down_w), locals_), row_w
    )

    def widen(values):
        return jnp.pad(
            values.reshape(locals_, held, -1), ((0, 0), (0, (nodes - 1) * cap), (0, 0))
        ).reshape(total, -1)

    partial_dx = (
        contract_last(gg, gate_w) + contract_last(gu, up_w)
        + contract_last(widen(sg), s_gate) + contract_last(widen(su), s_up)
    ).astype(bf16)
    score = jnp.sum(product, axis=1, keepdims=True)
    lane = jnp.arange(LANES)
    score = jnp.where(lane == expert, score, 0.0).astype(bf16)
    part = jnp.concatenate([partial_dx, score], axis=1).reshape(
        locals_, own_blocks + nodes - 1, cap, width + LANES
    )
    own_sum, home = reduce_rows(nodes, locals_, part)

    expert_grads = tuple(
        g.astype(bf16)[None]
        for g in (contract_first(rows_t, gg), contract_first(rows_t, gu),
                  contract_first(rows_g, flip(gh, locals_)))
    )
    piece = width // nodes
    start = n * piece
    here_t = own(lax.dynamic_slice_in_dim(rows_t, start, piece, 1))
    here_g = own(lax.dynamic_slice_in_dim(rows_g, start, piece, 1))
    every_t = jnp.concatenate([here_t, ext_t.reshape(-1, piece)], axis=0)
    every_g = jnp.concatenate([here_g, ext_g.reshape(-1, piece)], axis=0)
    packed = jnp.concatenate(packs, axis=0)
    shared_grads = (
        contract_first(every_t, packed[:, :units]).astype(bf16),
        contract_first(every_t, packed[:, units : 2 * units]).astype(bf16),
        contract_first(every_g, packed[:, 2 * units :]).astype(bf16),
    )

    own_rows = own_sum.reshape(held, width + LANES).astype(f32)
    home_rows = jnp.einsum("trc,rcd->td", rows, home[:, :, :width], preferred_element_type=f32)
    dx = (own_rows[:, :width] + home_rows).astype(bf16)
    home_score = jnp.sum(
        jnp.where(pick[:, 1:, :, None], home[None, :, :, width : width + E_NODE].astype(f32), 0.0),
        axis=2,
    )
    scores = jnp.concatenate([own_rows[:, None, width : width + E_NODE], home_score], axis=1)
    dgates = jnp.sum(jnp.where(named, scores[:, None], 0.0), axis=(2, 3))
    return (dx, dgates) + expert_grads + shared_grads


def solution(mesh):
    token = P(("node", "local"), None)
    routed = P("node", None, "local")
    shared = P(None, "local")
    shared_out = P("node", "local")
    return jax.shard_map(
        local,
        mesh=mesh,
        in_specs=(token,) * 4 + (routed,) * 3 + (shared,) * 3,
        out_specs=(token,) * 2 + (routed,) * 3 + (shared_out,) * 3,
        check_vma=False,
    )
```

```python
import functools

import jax
import jax.numpy as jnp
from jax import lax
from jax.experimental import pallas as pl
from jax.experimental.pallas import tpu as pltpu
from jax.sharding import PartitionSpec as P

E_NODE = 2
LANES = 128
MESH = pl.DeviceIdType.MESH


def bit_orders(local_count):
    bits = local_count.bit_length() - 1
    outer = list(range(1, bits))
    forward = [1 << b for b in outer] + [1]
    backward = [1 << b for b in outer[::-1]] + [1]
    return (forward, backward)


def near_first(node_count):
    return sorted(range(1, node_count), key=lambda s: min(s, node_count - s))


def greet(node_count, masks):
    n, l = lax.axis_index("node"), lax.axis_index("local")
    barrier = pltpu.get_barrier_semaphore()
    for r in range(1, node_count):
        pl.semaphore_signal(
            barrier, inc=1, device_id=(lax.rem(n + r, node_count), l), device_id_type=MESH
        )
    for mask in masks:
        pl.semaphore_signal(barrier, inc=1, device_id=(n, l ^ mask), device_id_type=MESH)
    pl.semaphore_wait(barrier, node_count - 1 + len(masks))


def gather_kernel(
    node_count, orders, tok, grad, sel_t, sel_g, meta,
    all_t, all_g, ext_t, ext_g, all_m, send_sem, recv_sem, own_sem,
):
    n, l = lax.axis_index("node"), lax.axis_index("local")
    forward, backward = orders
    stages = len(forward)
    own_blocks = tok.shape[0]
    part = ext_t.shape[-1]
    greet(node_count, forward)
    counter = [0]
    sends = []

    def remote(src, dst, device):
        i = counter[0]
        counter[0] += 1
        copy = pltpu.make_async_remote_copy(
            src_ref=src, dst_ref=dst, send_sem=send_sem.at[i], recv_sem=recv_sem.at[i],
            device_id=device, device_id_type=MESH,
        )
        copy.start()
        sends.append(copy)
        return copy

    fills = [
        pltpu.make_async_copy(tok, all_t.at[0, pl.ds(0, own_blocks)], own_sem.at[0]),
        pltpu.make_async_copy(grad, all_g.at[0, pl.ds(0, own_blocks)], own_sem.at[1]),
        pltpu.make_async_copy(meta.at[0], all_m.at[0, 0], own_sem.at[2]),
    ]
    for fill in fills:
        fill.start()

    def view(buf, s, start, size):
        if buf is all_t or buf is all_g:
            if s == 0:
                return buf.at[pl.ds(start, size), pl.ds(0, own_blocks)]
            return buf.at[pl.ds(start, size), own_blocks + s - 1]
        if buf is all_m:
            return buf.at[s, pl.ds(start, size)]
        return buf.at[s - 1, pl.ds(start, size)]

    arrived = {}
    order = near_first(node_count)
    for s in order:
        r = node_count - s
        m = lax.rem(n + r, node_count)
        columns = pl.ds(pl.multiple_of(m * part, LANES), part)
        arrived[s] = [
            remote(meta.at[r], all_m.at[s, 0], (m, l)),
            remote(sel_t.at[r - 1], all_t.at[0, own_blocks + s - 1], (m, l)),
            remote(sel_g.at[r - 1], all_g.at[0, own_blocks + s - 1], (m, l)),
            remote(tok.at[:, :, columns], ext_t.at[s - 1, 0], (m, l)),
            remote(grad.at[:, :, columns], ext_g.at[s - 1, 0], (m, l)),
        ]
    for fill in fills:
        fill.wait()

    items = [0] + order
    pending = {}

    def issue(item, stage):
        s = items[item]
        bufs = [(all_m, forward), (all_t, forward), (all_g, backward)]
        if s > 0:
            bufs += [(ext_t, forward), (ext_g, backward)]
        if stage > 0:
            before = pending[item]
        else:
            before = arrived.get(s, [])
        for copy in before:
            copy.wait_recv()
        size = 1 << stage
        pending[item] = [
            remote(view(buf, s, 0, size), view(buf, s, size, size), (n, l ^ bits[stage]))
            for buf, bits in bufs
        ]

    for tick in range(len(items) + stages - 1):
        for item in range(len(items)):
            stage = tick - item
            if 0 <= stage < stages:
                issue(item, stage)
    for item in range(len(items)):
        for copy in pending[item]:
            copy.wait_recv()
    for copy in sends:
        copy.wait_send()


def gather_rows(node_count, local_count, tok, grad, sel_t, sel_g, meta):
    own_blocks, cap, width = tok.shape
    orders = bit_orders(local_count)
    part = width // node_count
    copies = len(orders[0]) * (3 + 5 * (node_count - 1)) + 5 * (node_count - 1)
    rows = (local_count, own_blocks + node_count - 1, cap, width)
    ext = (node_count - 1, local_count, own_blocks, cap, part)
    bf16 = jnp.bfloat16
    vmem = pl.BlockSpec(memory_space=pltpu.VMEM)
    hbm = pl.BlockSpec(memory_space=pl.ANY)
    return pl.pallas_call(
        functools.partial(gather_kernel, node_count, orders),
        out_shape=[
            jax.ShapeDtypeStruct(rows, bf16),
            jax.ShapeDtypeStruct(rows, bf16),
            jax.ShapeDtypeStruct(ext, bf16),
            jax.ShapeDtypeStruct(ext, bf16),
            jax.ShapeDtypeStruct((node_count, local_count) + meta.shape[1:], bf16),
        ],
        in_specs=[vmem] * 5,
        out_specs=[hbm] * 5,
        scratch_shapes=[
            pltpu.SemaphoreType.DMA((copies,)),
            pltpu.SemaphoreType.DMA((copies,)),
            pltpu.SemaphoreType.DMA((3,)),
        ],
        compiler_params=pltpu.CompilerParams(collective_id=0, has_side_effects=True),
        name="gather_rows",
    )(tok, grad, sel_t, sel_g, meta)


def reduce_kernel(node_count, forward, own_blocks, part_ref, rows_t, rows_g, gg, gu, gh, pack,
                  own_ref, home_ref, packs, dw_g, dw_u, dw_d,
                  acc, land, back, held_t, held_g, grads,
                  send_sem, recv_sem, zsend_sem, zrecv_sem, psend_sem, precv_sem, load_sem, out_sem):
    n, l = lax.axis_index("node"), lax.axis_index("local")
    count, blocks, cap, width = part_ref.shape
    stages = len(forward)
    half = width // 2 // LANES * LANES
    load = pltpu.make_async_copy(part_ref, acc, load_sem.at[0])
    load.start()
    load_t = pltpu.make_async_copy(rows_t, held_t, load_sem.at[1])
    load_t.start()
    load_g = pltpu.make_async_copy(rows_g, held_g, load_sem.at[2])
    load_g.start()
    greet(node_count, forward)
    passed = []
    for s in near_first(node_count):
        copy = pltpu.make_async_remote_copy(
            src_ref=pack, dst_ref=packs.at[node_count - s - 1],
            send_sem=psend_sem.at[s - 1], recv_sem=precv_sem.at[node_count - s - 1],
            device_id=(lax.rem(n + s, node_count), l), device_id_type=MESH,
        )
        copy.start()
        passed.append(copy)
    load.wait()
    tile = 4 * LANES
    work = [(load_t, held_t, gg, dw_g), (None, held_t, gu, dw_u), (load_g, held_g, gh, dw_d)]
    stored = []

    def multiply(index):
        ready, held, right, out = work[index]
        if ready is not None:
            ready.wait()

        def step(c, carry):
            at = pl.ds(pl.multiple_of(c * tile, tile), tile)
            grads[index, at, :] = contract_first(held[:, at], right[...]).astype(jnp.bfloat16)
            return carry

        lax.fori_loop(0, held.shape[1] // tile, step, 0)
        copy = pltpu.make_async_copy(grads.at[index], out, out_sem.at[index])
        copy.start()
        stored.append(copy)

    groups = [(own_blocks, blocks - own_blocks), (0, own_blocks)]
    bands = [(0, half), (half, width - half)]
    top = stages - 1
    plans = [[top] + list(range(top))[::-1], [top] + list(range(top))]
    counter = [0]
    sends = []
    keep = {key: list(range(count)) for key in [(g, b) for g in range(2) for b in range(2)]}
    flight = {}

    def start(g, b, stage):
        bit = 1 << plans[b][stage]
        first, size = groups[g]
        columns = pl.ds(*bands[b])
        out = [p for p in keep[g, b] if p & bit]
        stay = [p for p in keep[g, b] if not p & bit]
        keep[g, b] = stay
        copies = []
        for p in out:
            i = counter[0]
            counter[0] += 1
            copy = pltpu.make_async_remote_copy(
                src_ref=acc.at[p, pl.ds(first, size), :, columns],
                dst_ref=land.at[p, pl.ds(first, size), :, columns],
                send_sem=send_sem.at[i], recv_sem=recv_sem.at[i],
                device_id=(n, l ^ forward[plans[b][stage]]), device_id_type=MESH,
            )
            copy.start()
            sends.append(copy)
            copies.append((p, copy))
        flight[g, b] = (bit, copies)

    def settle(g, b):
        first, size = groups[g]
        columns = pl.ds(*bands[b])
        bit, copies = flight[g, b]
        for p, copy in copies:
            copy.wait_recv()
            q = p ^ bit

            def add(k, carry, p=p, q=q):
                there = land[p, first + k, :, columns].astype(jnp.float32)
                here = acc[q, first + k, :, columns].astype(jnp.float32)
                acc[q, first + k, :, columns] = (here + there).astype(jnp.bfloat16)
                return carry

            lax.fori_loop(0, size, add, 0)

    homes = []
    for stage in range(stages + 1):
        for g in range(2):
            for b in range(2):
                if stage > 0:
                    settle(g, b)
                if stage < stages:
                    start(g, b, stage)
            if stage == stages and g == 0:
                for s in near_first(node_count):
                    copy = pltpu.make_async_remote_copy(
                        src_ref=acc.at[0, own_blocks + s - 1],
                        dst_ref=back.at[node_count - s - 1],
                        send_sem=zsend_sem.at[s - 1],
                        recv_sem=zrecv_sem.at[node_count - s - 1],
                        device_id=(lax.rem(n + s, node_count), l), device_id_type=MESH,
                    )
                    copy.start()
                    homes.append(copy)
        if stage < len(work):
            multiply(stage)
    for index in range(stages + 1, len(work)):
        multiply(index)
    own_ref[...] = acc[0, pl.ds(0, own_blocks)]
    for copy in homes:
        copy.wait_recv()
    home_ref[...] = back[...]
    for copy in passed:
        copy.wait_recv()
    for copy in sends + homes + passed:
        copy.wait_send()
    for copy in stored:
        copy.wait()


def reduce_rows(node_count, local_count, part, rows_t, rows_g, gg, gu, gh, pack):
    count, blocks, cap, width = part.shape
    forward = bit_orders(local_count)[0]
    own_blocks = blocks - (node_count - 1)
    bf16 = jnp.bfloat16
    vmem = pl.BlockSpec(memory_space=pltpu.VMEM)
    hbm = pl.BlockSpec(memory_space=pl.ANY)
    copies = 4 * (local_count - 1)
    grad = (rows_t.shape[1], gg.shape[1])
    return pl.pallas_call(
        functools.partial(reduce_kernel, node_count, forward, own_blocks),
        out_shape=[
            jax.ShapeDtypeStruct((own_blocks, cap, width), bf16),
            jax.ShapeDtypeStruct((node_count - 1, cap, width), bf16),
            jax.ShapeDtypeStruct((node_count - 1,) + pack.shape, bf16),
        ] + [jax.ShapeDtypeStruct(grad, bf16)] * 3,
        in_specs=[hbm] * 3 + [vmem] * 4,
        out_specs=[vmem] * 2 + [hbm] * 4,
        scratch_shapes=[
            pltpu.VMEM(part.shape, bf16),
            pltpu.VMEM(part.shape, bf16),
            pltpu.VMEM((node_count - 1, cap, width), bf16),
            pltpu.VMEM(rows_t.shape, bf16),
            pltpu.VMEM(rows_g.shape, bf16),
            pltpu.VMEM((3,) + grad, bf16),
            pltpu.SemaphoreType.DMA((copies,)),
            pltpu.SemaphoreType.DMA((copies,)),
            pltpu.SemaphoreType.DMA((node_count - 1,)),
            pltpu.SemaphoreType.DMA((node_count - 1,)),
            pltpu.SemaphoreType.DMA((node_count - 1,)),
            pltpu.SemaphoreType.DMA((node_count - 1,)),
            pltpu.SemaphoreType.DMA((3,)),
            pltpu.SemaphoreType.DMA((3,)),
        ],
        compiler_params=pltpu.CompilerParams(collective_id=1, has_side_effects=True),
        name="reduce_rows",
    )(part, rows_t, rows_g, gg, gu, gh, pack)


def silu_parts(pre_gate):
    sig = jax.nn.sigmoid(pre_gate)
    return (pre_gate * sig, sig * (1.0 + pre_gate * (1.0 - sig)))


def dot(left, right):
    return jnp.dot(left, right, preferred_element_type=jnp.float32)


def contract_first(left, right):
    return lax.dot_general(
        left, right, (((0,), (0,)), ((), ())), preferred_element_type=jnp.float32
    )


def contract_last(left, right):
    return lax.dot_general(
        left, right, (((1,), (1,)), ((), ())), preferred_element_type=jnp.float32
    )


def flip(values, local_count):
    bits = local_count.bit_length() - 1
    shaped = values.reshape((2,) * bits + (-1,) + values.shape[1:])
    axes = (0,) + tuple(range(1, bits))[::-1] + tuple(range(bits, shaped.ndim))
    return jnp.transpose(shaped, axes).reshape(values.shape)


def ffn_backward(pre_gate, pre_up, upstream, weight):
    activ, slope = silu_parts(pre_gate)
    hidden = activ * pre_up
    scaled = weight * upstream
    grad_up = (scaled * activ).astype(jnp.bfloat16)
    grad_gate = (scaled * pre_up * slope).astype(jnp.bfloat16)
    weighted = (weight * hidden).astype(jnp.bfloat16)
    return (grad_gate, grad_up, weighted, hidden * upstream)


def local(tokens, grad_out, gates, expert_ids, w_gate, w_up, w_down, s_gate, s_up, s_down):
    held, width = tokens.shape
    nodes, locals_ = lax.axis_size("node"), lax.axis_size("local")
    n, l = lax.axis_index("node"), lax.axis_index("local")
    cap = 2 * held // nodes
    own_blocks = held // cap
    bf16, f32 = jnp.bfloat16, jnp.float32

    rel = lax.rem(expert_ids // E_NODE - n + nodes, nodes)
    near = jnp.arange(nodes, dtype=jnp.int32)
    hit_k = rel[:, :, None] == near
    hit = jnp.any(hit_k, axis=1)
    lower = jnp.tril(jnp.ones((held, held), f32))
    rank = dot(lower, hit.astype(f32)).astype(jnp.int32) - 1
    slots = jnp.arange(cap, dtype=jnp.int32)
    pick = hit[:, :, None] & (rank[:, :, None] == slots)
    which = (lax.rem(expert_ids, E_NODE)[:, :, None] == jnp.arange(E_NODE)) & True
    named = hit_k[:, :, :, None] & which[:, :, None, :]
    weight = jnp.sum(jnp.where(named, gates.astype(f32)[:, :, None, None], 0.0), axis=1)
    rows = pick[:, 1:].astype(bf16)
    sel_t = jnp.einsum("trc,td->rcd", rows, tokens, preferred_element_type=f32).astype(bf16)
    sel_g = jnp.einsum("trc,td->rcd", rows, grad_out, preferred_element_type=f32).astype(bf16)
    slot_w = jnp.sum(jnp.where(pick[:, 1:, :, None], weight[:, 1:, None, :], 0.0), axis=0)
    meta = jnp.zeros((nodes, held, LANES), f32)
    meta = meta.at[0, :, :E_NODE].set(weight[:, 0])
    meta = meta.at[1:, :cap, :E_NODE].set(slot_w).astype(bf16)

    all_t, all_g, ext_t, ext_g, all_m = gather_rows(
        nodes, locals_,
        tokens.reshape(own_blocks, cap, width), grad_out.reshape(own_blocks, cap, width),
        sel_t, sel_g, meta,
    )
    total = locals_ * (held + (nodes - 1) * cap)
    rows_t, rows_g = all_t.reshape(total, width), all_g.reshape(total, width)
    units = s_gate.shape[1]

    def own(values):
        return values.reshape(locals_, -1, values.shape[-1])[:, :held].reshape(
            locals_ * held, values.shape[-1]
        )

    pre_gate, pre_up = dot(rows_t, s_gate), dot(rows_t, s_up)
    upstream = flip(dot(rows_g, s_down), locals_)
    sg, su, sh, _ = ffn_backward(own(pre_gate), own(pre_up), own(upstream), 1.0)
    pack = jnp.concatenate([sg, su, flip(sh, locals_)], axis=1)
    expert = l // (locals_ // E_NODE)
    table = jnp.concatenate([all_m[0, :, :, :E_NODE]] + [
        all_m[s, :, :cap, :E_NODE] for s in range(1, nodes)
    ], axis=1).reshape(total, E_NODE).astype(f32)
    mine = jnp.arange(E_NODE) == expert
    row_w = jnp.sum(jnp.where(mine, table, 0.0), axis=1, keepdims=True)
    gate_w, up_w, down_w = w_gate[0], w_up[0], w_down[0]
    gg, gu, gh, product = ffn_backward(
        dot(rows_t, gate_w), dot(rows_t, up_w), flip(dot(rows_g, down_w), locals_), row_w
    )

    def widen(values):
        return jnp.pad(
            values.reshape(locals_, held, -1), ((0, 0), (0, (nodes - 1) * cap), (0, 0))
        ).reshape(total, -1)

    partial_dx = (
        contract_last(gg, gate_w) + contract_last(gu, up_w)
        + contract_last(widen(sg), s_gate) + contract_last(widen(su), s_up)
    ).astype(bf16)
    score = jnp.sum(product, axis=1, keepdims=True)
    lane = jnp.arange(LANES)
    score = jnp.where(lane == expert, score, 0.0).astype(bf16)
    part = jnp.concatenate([partial_dx, score], axis=1).reshape(
        locals_, own_blocks + nodes - 1, cap, width + LANES
    )
    own_sum, home, packs, *dw = reduce_rows(
        nodes, locals_, part, rows_t, rows_g, gg, gu, flip(gh, locals_), pack
    )
    expert_grads = tuple(g[None] for g in dw)
    piece = width // nodes
    start = n * piece
    here_t = own(lax.dynamic_slice_in_dim(rows_t, start, piece, 1))
    here_g = own(lax.dynamic_slice_in_dim(rows_g, start, piece, 1))
    every_t = jnp.concatenate([here_t, ext_t.reshape(-1, piece)], axis=0)
    every_g = jnp.concatenate([here_g, ext_g.reshape(-1, piece)], axis=0)
    packed = jnp.concatenate([pack, packs.reshape(-1, pack.shape[1])], axis=0)
    shared_grads = (
        contract_first(every_t, packed[:, :units]).astype(bf16),
        contract_first(every_t, packed[:, units : 2 * units]).astype(bf16),
        contract_first(every_g, packed[:, 2 * units :]).astype(bf16),
    )

    own_rows = own_sum.reshape(held, width + LANES).astype(f32)
    home_rows = jnp.einsum("trc,rcd->td", rows, home[:, :, :width], preferred_element_type=f32)
    dx = (own_rows[:, :width] + home_rows).astype(bf16)
    home_score = jnp.sum(
        jnp.where(pick[:, 1:, :, None], home[None, :, :, width : width + E_NODE].astype(f32), 0.0),
        axis=2,
    )
    scores = jnp.concatenate([own_rows[:, None, width : width + E_NODE], home_score], axis=1)
    dgates = jnp.sum(jnp.where(named, scores[:, None], 0.0), axis=(2, 3))
    return (dx, dgates) + expert_grads + shared_grads


def solution(mesh):
    token = P(("node", "local"), None)
    routed = P("node", None, "local")
    shared = P(None, "local")
    shared_out = P("node", "local")
    return jax.shard_map(
        local,
        mesh=mesh,
        in_specs=(token,) * 4 + (routed,) * 3 + (shared,) * 3,
        out_specs=(token,) * 2 + (routed,) * 3 + (shared_out,) * 3,
        check_vma=False,
    )
```
